32 devices in a mesh: row: 4 (over y, core), col: 8 (over z, x).
Axes of the slice: x: 2, y: 2, z: 4, core: 2. Of those that a mesh axis runs over, the one named last changes fastest.
Arguments:
- tokens: bfloat16 [256, 2, 4096], P(None, None, 'row'), may hold values from -6 to 6
- task_emb: bfloat16 [512, 1024], replicated, may hold values from -6 to 6
- gen_in: bfloat16 [1024, 512], replicated, may hold values from -0.1875 to 0.1875
- gen_a: bfloat16 [512, 4096, 16], P(None, ('row', 'col')), may hold values from -0.0078125 to 0.0078125
- gen_b: bfloat16 [512, 16, 14336], P(None, 'row', 'col'), may hold values from -0.125 to 0.125
- w_gate: bfloat16 [4096, 14336], P('row', 'col'), may hold values from -0.09375 to 0.09375
- w_up: bfloat16 [4096, 14336], P('row', 'col'), may hold values from -0.09375 to 0.09375
- w_down: bfloat16 [14336, 4096], P('col', 'row'), may hold values from -0.046875 to 0.046875
- group_count: int32 [64], replicated, may hold values from 1 to 16, 256 in all
- group_task: int32 [64], replicated, may hold values from 0 to 511, as said below
Outputs:
- mixed: bfloat16 [256, 2, 4096], P('col', None, 'row')
The draws below stay inside these ranges and needn't reach their ends.
Inputs may be any that keep to these rules, and one draw needn't show every extreme that they name: `group_count`: requests in each group, in the order of the requests; they sum to 256 and the largest is 16. `group_task`: distinct task ids, one for each group.
All inputs are finite; a program needn't handle non-finite values.
Results may differ from the reference program's by a relative error of at most 0.0078.
Values may be sent and summed in bfloat16 or wider, within the bound.
A program may use at most 128 MiB of HBM per device.

```python
import math
import jax
import jax.numpy as jnp
import numpy as np

D = 4096
HIDDEN_UNITS = 14336
RANK = 16
EMB = 1024
HYPER = 512
TASKS = 512
GROUPS = 64
MOST = 16
REQUEST_COUNT = 256
DRAFT_TOKENS = 2


def draw_group_task(key, part):
    return jax.random.permutation(key, TASKS)[:GROUPS].astype(jnp.int32)


def block_levels(stream_key, shape, cuts, least, high):
    def one(dim, blocks):
        draws = jax.random.uniform(jax.random.fold_in(jax.random.fold_in(stream_key, 6), dim), (blocks,), jnp.float32, least / len(cuts), high / len(cuts))
        return jnp.repeat(jnp.exp(draws), shape[dim] // blocks).reshape((-1,) + (1,) * (len(shape) - dim - 1))

    level = one(*cuts[0])
    for cut in cuts[1:]:
        level = level * one(*cut)
    return level


def length_profile(number_of, total, limit, skew):
    weights = [(1 << 20) // math.isqrt(rank ** skew) + 1 for rank in range(2, number_of + 1)]
    rest, given = total - limit - (number_of - 1), [1] * (number_of - 1)
    while rest > 0:
        movable = [i for i in range(number_of - 1) if given[i] < limit]
        whole, budget = sum([weights[i] for i in movable]), rest
        for i in movable:
            addition = min(limit - given[i], max(1, budget * weights[i] // whole), rest)
            given[i] = given[i] + addition
            rest = rest - addition
    return np.array([limit] + given)


def uneven(own_key, number_of, total, limit, skew):
    if number_of == 2:
        one = jax.random.randint(own_key, (), max(1, total - limit), min(limit, total - 1) + 1)
        return jnp.stack([one, total - one])
    tallies = jnp.asarray(length_profile(number_of, total, limit, skew), jnp.int32)
    couples = (number_of - 1) // 2
    giver, sink = tallies[1:1 + 2 * couples:2], tallies[2:2 + 2 * couples:2]
    room = jnp.minimum(giver - 1, limit - sink)
    passed = jax.random.randint(jax.random.fold_in(own_key, 1), (couples,), 0, 1 << 20) % (room + 1)
    tallies = tallies.at[1:1 + 2 * couples:2].set(giver - passed).at[2:2 + 2 * couples:2].set(sink + passed)
    return tallies[jax.random.permutation(jax.random.fold_in(own_key, 2), number_of)]


def scatter_about(key, extent, width, reach, shards=(), kind=jnp.bfloat16):
    entries = jax.random.normal(key, extent, jnp.float32) * width
    if len(shards) > 0:
        entries = block_levels(key, extent, shards, -0.22, 0.18) * entries
    return jnp.clip(entries, min=-reach, max=reach).astype(kind)


def setup_inputs(seed: int = 0) -> dict:
    arg_keys = jax.random.split(jax.random.key(seed), 11)
    tokens = scatter_about(arg_keys[0], (REQUEST_COUNT, DRAFT_TOKENS, D), 1.0, 6.0, ((2, 4),))
    task_emb = scatter_about(arg_keys[1], (TASKS, EMB), 1.0, 6.0)
    gen_in = scatter_about(arg_keys[2], (EMB, HYPER), EMB ** -0.5, 0.1875)
    gen_a = scatter_about(arg_keys[3], (HYPER, D, RANK), (HYPER * D // 4) ** -0.5, 0.0078125, ((1, 32),))
    gen_b = scatter_about(arg_keys[4], (HYPER, RANK, HIDDEN_UNITS), (HYPER * RANK // 4) ** -0.5, 0.125, ((1, 4), (2, 8)))
    w_gate = scatter_about(arg_keys[5], (D, HIDDEN_UNITS), D ** -0.5, 0.09375, ((0, 4), (1, 8)))
    w_up = scatter_about(arg_keys[6], (D, HIDDEN_UNITS), D ** -0.5, 0.09375, ((0, 4), (1, 8)))
    w_down = scatter_about(arg_keys[7], (HIDDEN_UNITS, D), HIDDEN_UNITS ** -0.5, 0.046875, ((0, 8), (1, 4)))
    group_count = uneven(arg_keys[8], GROUPS, REQUEST_COUNT, MOST, 2).astype(jnp.int32)
    group_task = draw_group_task(jax.random.fold_in(arg_keys[10], 71), 0)
    return {"tokens": tokens, "task_emb": task_emb, "gen_in": gen_in, "gen_a": gen_a, "gen_b": gen_b, "w_gate": w_gate, "w_up": w_up, "w_down": w_down, "group_count": group_count, "group_task": group_task}


def reference(tokens, task_emb, gen_in, gen_a, gen_b, w_gate, w_up, w_down, group_count, group_task):
    group_ends = jnp.cumsum(group_count).astype(jnp.int32)
    request_ids = jnp.arange(REQUEST_COUNT, dtype=jnp.int32)
    request_group = jnp.sum((request_ids[:, None] >= group_ends[None, :]).astype(jnp.int32), axis=1).astype(jnp.int32)
    chosen = task_emb[group_task]
    hyper_out = jax.nn.silu(jnp.dot(chosen, gen_in, preferred_element_type=jnp.float32)).astype(jnp.bfloat16)
    factor_a = jnp.dot(hyper_out, gen_a.reshape(HYPER, D * RANK), preferred_element_type=jnp.float32).astype(jnp.bfloat16).reshape(GROUPS, D, RANK)
    second_factor = jnp.dot(hyper_out, gen_b.reshape(HYPER, RANK * HIDDEN_UNITS), preferred_element_type=jnp.float32).astype(jnp.bfloat16).reshape(GROUPS, RANK, HIDDEN_UNITS)
    flat_tokens = tokens.reshape(REQUEST_COUNT * DRAFT_TOKENS, D)
    gate_total = jnp.dot(flat_tokens, w_gate, preferred_element_type=jnp.float32)
    up_total = jnp.dot(flat_tokens, w_up, preferred_element_type=jnp.float32)
    reduced_rank_term = jnp.einsum("bsd,bdr->bsr", tokens.astype(jnp.float32), factor_a[request_group].astype(jnp.float32)).astype(jnp.bfloat16)
    adapter_update = jnp.einsum("klv,kve->kle", reduced_rank_term.astype(jnp.float32), second_factor[request_group].astype(jnp.float32))
    adapter_update = adapter_update.reshape(REQUEST_COUNT * DRAFT_TOKENS, HIDDEN_UNITS)
    hidden_state = (jax.nn.silu(gate_total) * (up_total + adapter_update)).astype(jnp.bfloat16)
    mixed = jnp.dot(hidden_state, w_down, preferred_element_type=jnp.float32).astype(jnp.bfloat16)
    return mixed.reshape(REQUEST_COUNT, DRAFT_TOKENS, D)
```

```python
import jax
import jax.numpy as jnp
from jax import lax
from jax.sharding import PartitionSpec as P


def shards(tokens, task_emb, gen_in, gen_a, gen_b, w_gate, w_up, w_down, group_count, group_task):
    batch_size, draft_len, width_part = tokens.shape
    row_count = batch_size * draft_len
    flat_tokens = tokens.reshape(row_count, width_part)
    groups = group_count.shape[0]
    group_ends = jnp.cumsum(group_count)
    group_starts = group_ends - group_count
    request_ids = jnp.arange(row_count, dtype=jnp.int32) // draft_len
    member_rows = (request_ids[:, None] >= group_starts[None, :]) & (
        request_ids[:, None] < group_ends[None, :]
    )
    chosen = jnp.take(task_emb, group_task, axis=0)
    hyper_out = jax.nn.silu(jnp.dot(chosen, gen_in, preferred_element_type=jnp.float32)).astype(
        jnp.bfloat16
    )
    hyper_width, slab_width, rank_dim = gen_a.shape
    a_local = lax.dot_general(
        gen_a, hyper_out, (((0,), (1,)), ((), ())), preferred_element_type=jnp.float32
    ).astype(jnp.bfloat16)
    a_local = a_local.transpose(0, 1, 2).reshape(slab_width, rank_dim * groups)
    col = lax.axis_index("col")
    own = lax.dynamic_slice_in_dim(flat_tokens, col * slab_width, slab_width, axis=1)
    wide_low = jnp.dot(own, a_local, preferred_element_type=jnp.float32)
    low_part = jnp.sum(
        wide_low.reshape(row_count, rank_dim, groups)
        * member_rows.astype(jnp.float32)[:, None, :],
        axis=2,
    )
    low_half = lax.psum(low_part, ("row", "col")).astype(jnp.bfloat16)
    _, rank_part, ff_part = gen_b.shape
    row = lax.axis_index("row")
    low_own = lax.dynamic_slice_in_dim(low_half, row * rank_part, rank_part, axis=1)
    b_local = lax.dot_general(
        gen_b, hyper_out, (((0,), (1,)), ((), ())), preferred_element_type=jnp.float32
    ).astype(jnp.bfloat16)
    spread = jnp.where(member_rows[:, None, :], low_own[:, :, None], jnp.bfloat16(0))
    lora_part = lax.dot_general(
        spread, b_local, (((1, 2), (0, 2)), ((), ())), preferred_element_type=jnp.float32
    )
    gate_part = jnp.dot(flat_tokens, w_gate, preferred_element_type=jnp.float32)
    up_part = jnp.dot(flat_tokens, w_up, preferred_element_type=jnp.float32) + lora_part
    both = jnp.stack([gate_part, up_part]).astype(jnp.bfloat16)
    both = lax.psum_scatter(both, "row", scatter_dimension=1, tiled=True).astype(jnp.float32)
    hidden_own = (jax.nn.silu(both[0]) * both[1]).astype(jnp.bfloat16)
    hidden_state = lax.all_gather(hidden_own, "row", axis=0, tiled=True)
    mixed = lax.psum_scatter(
        jnp.dot(hidden_state, w_down, preferred_element_type=jnp.float32).astype(jnp.bfloat16),
        "col",
        scatter_dimension=0,
        tiled=True,
    )
    col_count = lax.axis_size("col")
    return mixed.reshape(batch_size // col_count, draft_len, w_down.shape[1])


def solution(mesh):
    in_specs = (
        P(None, None, "row"),
        P(),
        P(),
        P(None, ("row", "col"), None),
        P(None, "row", "col"),
        P("row", "col"),
        P("row", "col"),
        P("col", "row"),
        P(),
        P(),
    )
    out_specs = P("col", None, "row")
    return jax.shard_map(shards, mesh=mesh, in_specs=in_specs, out_specs=out_specs, check_vma=False)
```

```python
import functools

import jax
import jax.numpy as jnp
from jax import lax
from jax.experimental import pallas as pl
from jax.experimental.pallas import tpu as pltpu
from jax.sharding import PartitionSpec as P

SUBROWS = 16


def tile_of(width):
    return 256 if width % 256 == 0 else 128


def layer_kernel(
    row_count, col_count, chunks,
    tok, spread, b_own, w_gate, w_up, w_down, out,
    part32, part16, pair_in, y_out, y_in, hid, mix32, mix16, x_in, z_out, z_in,
    pair_ss, pair_rs, y_ss, y_rs, ag_ss, ag_rs, fw_ss, fw_rs, x_ss, x_rs, z_ss, z_rs,
):
    row, col = lax.axis_index("row"), lax.axis_index("col")
    ys, zs = row_count // 2, col_count // 2
    y, core = row // 2, row % 2
    z, x = col // 2, col % 2
    rows = tok.shape[0] // chunks
    half = rows // 2
    piece = half // ys
    sub = half // zs
    ff = w_gate.shape[1]
    model = w_down.shape[1]

    row_pair = {"row": y * 2 + (1 - core)}
    col_pair = {"col": z * 2 + (1 - x)}
    y_peer = [{"row": ((y + q) % ys) * 2 + core} for q in range(1, ys)]
    z_peer = [{"col": ((z + q) % zs) * 2 + x} for q in range(1, zs)]

    barrier = pltpu.get_barrier_semaphore()
    everyone = [row_pair, col_pair] + y_peer + z_peer
    for peer in everyone:
        pl.semaphore_signal(
            barrier, inc=1, device_id=peer, device_id_type=pl.DeviceIdType.MESH
        )
    pl.semaphore_wait(barrier, len(everyone))

    sent = []

    def send(src, dst, ssem, rsem, peer):
        copy = pltpu.make_async_remote_copy(
            src_ref=src, dst_ref=dst, send_sem=ssem, recv_sem=rsem,
            device_id=peer, device_id_type=pl.DeviceIdType.MESH,
        )
        copy.start()
        sent.append(copy)
        return copy

    def at(start, size):
        return pl.ds(pl.multiple_of(start, SUBROWS), size)

    mine, other = at(core * half, half), at((1 - core) * half, half)
    own = at(core * half + y * piece, piece)
    x_mine, x_other = at(x * half, half), at((1 - x) * half, half)
    pair_c, y_c, ag_c, fw_c, x_c, z_c = {}, {}, {}, {}, {}, {}

    def gate_up(k):
        here = pl.ds(k * rows, rows)
        width = tile_of(ff)

        def body(n, carry):
            lo = pl.ds(pl.multiple_of(n * width, 128), width)
            hi = pl.ds(pl.multiple_of(ff + n * width, 128), width)
            gate = jnp.dot(tok[here, :], w_gate[:, lo], preferred_element_type=jnp.float32)
            up = jnp.dot(tok[here, :], w_up[:, lo], preferred_element_type=jnp.float32)
            up += jnp.dot(spread[here, :], b_own[:, lo], preferred_element_type=jnp.float32)
            part32[k, :, lo] = gate
            part32[k, :, hi] = up
            part16[k, :, lo] = gate.astype(jnp.bfloat16)
            part16[k, :, hi] = up.astype(jnp.bfloat16)
            return carry

        lax.fori_loop(0, ff // width, body, 0)
        pair_c[k] = send(part16.at[k, other], pair_in.at[k], pair_ss.at[k], pair_rs.at[k], row_pair)

    def add_pair(k):
        pair_c[k].wait_recv()
        total = part32[k, mine, :] + pair_in[k].astype(jnp.float32)
        part32[k, mine, :] = total
        y_out[k] = total.astype(jnp.bfloat16)
        y_c[k] = [
            send(
                y_out.at[k, at(((y + q) % ys) * piece, piece)], y_in.at[k, q - 1],
                y_ss.at[k, q - 1], y_rs.at[k, q - 1], y_peer[q - 1],
            )
            for q in range(1, ys)
        ]

    def activate(k):
        total = part32[k, own, :]
        for q in range(ys - 1):
            y_c[k][q].wait_recv()
            total += y_in[k, q].astype(jnp.float32)
        hid[k, own, :] = (jax.nn.silu(total[:, :ff]) * total[:, ff:]).astype(jnp.bfloat16)
        ag_c[k] = [
            send(hid.at[k, own], hid.at[k, own], ag_ss.at[k, q], ag_rs.at[k, q], y_peer[q])
            for q in range(ys - 1)
        ]

    def forward(k):
        for q in range(ys - 1):
            ag_c[k][q].wait_recv()
        fw_c[k] = send(hid.at[k, mine], hid.at[k, mine], fw_ss.at[k], fw_rs.at[k], row_pair)

    def down(k):
        fw_c[k].wait_recv()
        width = tile_of(model)

        def body(n, carry):
            lo = pl.ds(pl.multiple_of(n * width, 128), width)
            mix = jnp.dot(hid[k], w_down[:, lo], preferred_element_type=jnp.float32)
            mix32[k, :, lo] = mix
            mix16[k, :, lo] = mix.astype(jnp.bfloat16)
            return carry

        lax.fori_loop(0, model // width, body, 0)
        x_c[k] = send(mix16.at[k, x_other], x_in.at[k], x_ss.at[k], x_rs.at[k], col_pair)

    def add_x(k):
        x_c[k].wait_recv()
        total = mix32[k, x_mine, :] + x_in[k].astype(jnp.float32)
        mix32[k, x_mine, :] = total
        z_out[k] = total.astype(jnp.bfloat16)
        z_c[k] = [
            send(
                z_out.at[k, at(((z + q) % zs) * sub, sub)], z_in.at[k, q - 1],
                z_ss.at[k, q - 1], z_rs.at[k, q - 1], z_peer[q - 1],
            )
            for q in range(1, zs)
        ]

    def finish(k):
        total = mix32[k, at(x * half + z * sub, sub), :]
        for q in range(zs - 1):
            z_c[k][q].wait_recv()
            total += z_in[k, q].astype(jnp.float32)
        out[pl.ds(k * sub, sub), :] = total.astype(jnp.bfloat16)

    front = ((gate_up, 0), (add_pair, 1))
    middle = ((activate, 0),)
    back = ((forward, 0), (down, 1), (add_x, 2), (finish, 3))
    for stages in (front, middle, back):
        for step in range(chunks + stages[-1][1]):
            for stage, lag in stages:
                if 0 <= step - lag < chunks:
                    stage(step - lag)
    for copy in sent:
        copy.wait_send()


def shards(
    row_count, col_count,
    tokens, task_emb, gen_in, gen_a, gen_b, w_gate, w_up, w_down, group_count, group_task,
):
    batch_size, draft_len, width_part = tokens.shape
    total_rows = batch_size * draft_len
    groups = group_count.shape[0]
    chunks = total_rows // (col_count * SUBROWS)
    ys, zs = row_count // 2, col_count // 2

    def reorder(array):
        cut = array.reshape(zs, 2, chunks, SUBROWS, array.shape[-1])
        return cut.transpose(2, 1, 0, 3, 4).reshape(total_rows, array.shape[-1])

    flat_tokens = reorder(tokens)
    group_ends = jnp.cumsum(group_count)
    group_starts = group_ends - group_count
    request_ids = reorder(jnp.arange(total_rows, dtype=jnp.int32)[:, None] // draft_len)
    member_rows = (request_ids >= group_starts[None, :]) & (request_ids < group_ends[None, :])
    chosen = jnp.take(task_emb, group_task, axis=0)
    hyper_out = jax.nn.silu(jnp.dot(chosen, gen_in, preferred_element_type=jnp.float32)).astype(
        jnp.bfloat16
    )
    hyper_width, slab_width, rank_dim = gen_a.shape
    a_local = lax.dot_general(
        gen_a, hyper_out, (((0,), (1,)), ((), ())), preferred_element_type=jnp.float32
    ).astype(jnp.bfloat16)
    a_local = a_local.reshape(slab_width, rank_dim * groups)
    col, row = lax.axis_index("col"), lax.axis_index("row")
    own = lax.dynamic_slice_in_dim(flat_tokens, col * slab_width, slab_width, axis=1)
    wide_low = jnp.dot(own, a_local, preferred_element_type=jnp.float32)
    low_part = jnp.sum(
        wide_low.reshape(total_rows, rank_dim, groups)
        * member_rows.astype(jnp.float32)[:, None, :],
        axis=2,
    )
    low_half = lax.psum(low_part, ("row", "col")).astype(jnp.bfloat16)
    _, rank_part, ff = gen_b.shape
    low_own = lax.dynamic_slice_in_dim(low_half, row * rank_part, rank_part, axis=1)
    b_own = lax.dot_general(
        hyper_out, gen_b, (((1,), (0,)), ((), ())), preferred_element_type=jnp.float32
    ).astype(jnp.bfloat16)
    b_own = b_own.transpose(1, 0, 2).reshape(rank_part * groups, ff)
    spread = jnp.where(
        jnp.tile(member_rows, (1, rank_part)), jnp.repeat(low_own, groups, axis=1), jnp.bfloat16(0)
    )
    model = w_down.shape[1]
    rows = total_rows // chunks
    half = rows // 2
    bf, f32 = jnp.bfloat16, jnp.float32
    dma = pltpu.SemaphoreType.DMA
    y_sems, z_sems = max(ys - 1, 1), max(zs - 1, 1)
    vmem = pl.BlockSpec(memory_space=pltpu.VMEM)
    mixed = pl.pallas_call(
        functools.partial(layer_kernel, row_count, col_count, chunks),
        out_shape=jax.ShapeDtypeStruct((total_rows // col_count, model), bf),
        in_specs=[vmem] * 6,
        out_specs=vmem,
        scratch_shapes=[
            pltpu.VMEM((chunks, rows, 2 * ff), f32),
            pltpu.VMEM((chunks, rows, 2 * ff), bf),
            pltpu.VMEM((chunks, half, 2 * ff), bf),
            pltpu.VMEM((chunks, half, 2 * ff), bf),
            pltpu.VMEM((chunks, y_sems, half // ys, 2 * ff), bf),
            pltpu.VMEM((chunks, rows, ff), bf),
            pltpu.VMEM((chunks, rows, model), f32),
            pltpu.VMEM((chunks, rows, model), bf),
            pltpu.VMEM((chunks, half, model), bf),
            pltpu.VMEM((chunks, half, model), bf),
            pltpu.VMEM((chunks, z_sems, half // zs, model), bf),
            dma((chunks,)), dma((chunks,)),
            dma((chunks, y_sems)), dma((chunks, y_sems)),
            dma((chunks, y_sems)), dma((chunks, y_sems)),
            dma((chunks,)), dma((chunks,)),
            dma((chunks,)), dma((chunks,)),
            dma((chunks, z_sems)), dma((chunks, z_sems)),
        ],
        compiler_params=pltpu.CompilerParams(
            collective_id=0, has_side_effects=True, vmem_limit_bytes=60 * 1024 * 1024
        ),
        name="layer",
    )(flat_tokens, spread, b_own, w_gate, w_up, w_down)
    return mixed.reshape(batch_size // col_count, draft_len, model)


def solution(mesh):
    in_specs = (
        P(None, None, "row"),
        P(),
        P(),
        P(None, ("row", "col"), None),
        P(None, "row", "col"),
        P("row", "col"),
        P("row", "col"),
        P("col", "row"),
        P(),
        P(),
    )
    out_specs = P("col", None, "row")
    body = functools.partial(shards, mesh.shape["row"], mesh.shape["col"])
    return jax.shard_map(body, mesh=mesh, in_specs=in_specs, out_specs=out_specs, check_vma=False)
```

```python
import functools

import jax
import jax.numpy as jnp
from jax import lax
from jax.experimental import pallas as pl
from jax.experimental.pallas import tpu as pltpu
from jax.sharding import PartitionSpec as P

SUBROWS = 16


def tile_of(width):
    return 256 if width % 256 == 0 else 128


def layer_kernel(
    row_count, col_count, chunks,
    tok, low_part, member, b_own, w_gate, w_up, w_down, out,
    spread, low_in, low_row, low_all, part32, part16, pair_in, y_out, y_in, hid, mix32, mix16, x_in, z_out, z_in,
    lr_ss, lr_rs, lc_ss, lc_rs, pair_ss, pair_rs, y_ss, y_rs, ag_ss, ag_rs, fw_ss, fw_rs, x_ss, x_rs, z_ss, z_rs,
):
    row, col = lax.axis_index("row"), lax.axis_index("col")
    ys, zs = row_count // 2, col_count // 2
    y, core = row // 2, row % 2
    z, x = col // 2, col % 2
    rows = tok.shape[0] // chunks
    half = rows // 2
    piece = half // ys
    sub = half // zs
    ff = w_gate.shape[1]
    model = w_down.shape[1]

    row_pair = {"row": y * 2 + (1 - core)}
    col_pair = {"col": z * 2 + (1 - x)}
    y_peer = [{"row": ((y + q) % ys) * 2 + core} for q in range(1, ys)]
    z_peer = [{"col": ((z + q) % zs) * 2 + x} for q in range(1, zs)]

    barrier = pltpu.get_barrier_semaphore()
    row_peer = [{"row": (row + q) % row_count} for q in range(1, row_count)]
    col_peer = [{"col": (col + q) % col_count} for q in range(1, col_count)]
    everyone = row_peer + col_peer
    for peer in everyone:
        pl.semaphore_signal(
            barrier, inc=1, device_id=peer, device_id_type=pl.DeviceIdType.MESH
        )
    pl.semaphore_wait(barrier, len(everyone))

    sent = []

    def send(src, dst, ssem, rsem, peer):
        copy = pltpu.make_async_remote_copy(
            src_ref=src, dst_ref=dst, send_sem=ssem, recv_sem=rsem,
            device_id=peer, device_id_type=pl.DeviceIdType.MESH,
        )
        copy.start()
        sent.append(copy)
        return copy

    def at(start, size):
        return pl.ds(pl.multiple_of(start, SUBROWS), size)

    mine, other = at(core * half, half), at((1 - core) * half, half)
    own = at(core * half + y * piece, piece)
    x_mine, x_other = at(x * half, half), at((1 - x) * half, half)
    pair_c, y_c, ag_c, fw_c, x_c, z_c = {}, {}, {}, {}, {}, {}

    low_row_c = [
        send(
            low_part.at[(row + q) % row_count], low_in.at[q - 1],
            lr_ss.at[q - 1], lr_rs.at[q - 1], row_peer[q - 1],
        )
        for q in range(1, row_count)
    ]
    low_col_c = []

    def low_over_row():
        total = low_part[row]
        for q in range(row_count - 1):
            low_row_c[q].wait_recv()
            total += low_in[q]
        low_row[...] = total
        for q in range(col_count - 1):
            low_col_c.append(
                send(low_row, low_all.at[q], lc_ss.at[q], lc_rs.at[q], col_peer[q])
            )

    def low_over_col():
        total = low_row[...]
        for q in range(col_count - 1):
            low_col_c[q].wait_recv()
            total += low_all[q]
        total = total.astype(jnp.bfloat16).astype(jnp.float32)
        wide = [member[...] * total[r : r + 1, :] for r in range(total.shape[0])]
        spread[...] = jnp.concatenate(wide, axis=0).T.astype(jnp.bfloat16)

    def partial(k, which):
        here = pl.ds(k * rows, rows)
        width = tile_of(ff)
        j = 2 * k + which

        def body(n, carry):
            lo = pl.ds(pl.multiple_of(n * width, 128), width)
            weights = w_up if which else w_gate
            part = jnp.dot(tok[here, :], weights[:, lo], preferred_element_type=jnp.float32)
            if which:
                part += jnp.dot(spread[here, :], b_own[:, lo], preferred_element_type=jnp.float32)
            part32[j, :, lo] = part
            part16[j, :, lo] = part.astype(jnp.bfloat16)
            return carry

        lax.fori_loop(0, ff // width, body, 0)
        pair_c[j] = send(part16.at[j, other], pair_in.at[j], pair_ss.at[j], pair_rs.at[j], row_pair)

    def add_pair(j):
        pair_c[j].wait_recv()
        total = part32[j, mine, :] + pair_in[j].astype(jnp.float32)
        part32[j, mine, :] = total
        y_out[j] = total.astype(jnp.bfloat16)
        y_c[j] = [
            send(
                y_out.at[j, at(((y + q) % ys) * piece, piece)], y_in.at[j, q - 1],
                y_ss.at[j, q - 1], y_rs.at[j, q - 1], y_peer[q - 1],
            )
            for q in range(1, ys)
        ]

    def summed(j):
        total = part32[j, own, :]
        for q in range(ys - 1):
            y_c[j][q].wait_recv()
            total += y_in[j, q].astype(jnp.float32)
        return total

    def activate(k):
        gate, up = summed(2 * k), summed(2 * k + 1)
        hid[k, own, :] = (jax.nn.silu(gate) * up).astype(jnp.bfloat16)
        ag_c[k] = [
            send(hid.at[k, own], hid.at[k, own], ag_ss.at[k, q], ag_rs.at[k, q], y_peer[q])
            for q in range(ys - 1)
        ]

    def forward(k):
        for q in range(ys - 1):
            ag_c[k][q].wait_recv()
        fw_c[k] = send(hid.at[k, mine], hid.at[k, mine], fw_ss.at[k], fw_rs.at[k], row_pair)

    def down(k):
        fw_c[k].wait_recv()
        width = tile_of(model)

        def body(n, carry):
            lo = pl.ds(pl.multiple_of(n * width, 128), width)
            mix = jnp.dot(hid[k], w_down[:, lo], preferred_element_type=jnp.float32)
            mix32[k, :, lo] = mix
            mix16[k, :, lo] = mix.astype(jnp.bfloat16)
            return carry

        lax.fori_loop(0, model // width, body, 0)
        x_c[k] = send(mix16.at[k, x_other], x_in.at[k], x_ss.at[k], x_rs.at[k], col_pair)

    def add_x(k):
        x_c[k].wait_recv()
        total = mix32[k, x_mine, :] + x_in[k].astype(jnp.float32)
        mix32[k, x_mine, :] = total
        z_out[k] = total.astype(jnp.bfloat16)
        z_c[k] = [
            send(
                z_out.at[k, at(((z + q) % zs) * sub, sub)], z_in.at[k, q - 1],
                z_ss.at[k, q - 1], z_rs.at[k, q - 1], z_peer[q - 1],
            )
            for q in range(1, zs)
        ]

    def finish(k):
        total = mix32[k, at(x * half + z * sub, sub), :]
        for q in range(zs - 1):
            z_c[k][q].wait_recv()
            total += z_in[k, q].astype(jnp.float32)
        out[pl.ds(k * sub, sub), :] = total.astype(jnp.bfloat16)

    middle = ((activate, 0),)
    back = ((forward, 0), (down, 1), (add_x, 2), (finish, 3))
    order = [(k, 0) for k in range(chunks)] + [(k, 1) for k in range(chunks)]
    for i, (k, which) in enumerate(order):
        if which and k == 0:
            low_over_col()
        partial(k, which)
        if i == 0:
            low_over_row()
        else:
            before = order[i - 1]
            add_pair(2 * before[0] + before[1])
    add_pair(2 * chunks - 1)
    for stages in (middle, back):
        for step in range(chunks + stages[-1][1]):
            for stage, lag in stages:
                if 0 <= step - lag < chunks:
                    stage(step - lag)
    for copy in sent:
        copy.wait_send()


def shards(
    row_count, col_count,
    tokens, task_emb, gen_in, gen_a, gen_b, w_gate, w_up, w_down, group_count, group_task,
):
    batch_size, draft_len, width_part = tokens.shape
    total_rows = batch_size * draft_len
    groups = group_count.shape[0]
    chunks = total_rows // (col_count * SUBROWS)
    ys, zs = row_count // 2, col_count // 2

    def reorder(array):
        cut = array.reshape(zs, 2, chunks, SUBROWS, array.shape[-1])
        return cut.transpose(2, 1, 0, 3, 4).reshape(total_rows, array.shape[-1])

    flat_tokens = reorder(tokens)
    group_ends = jnp.cumsum(group_count)
    group_starts = group_ends - group_count
    request_ids = reorder(jnp.arange(total_rows, dtype=jnp.int32)[:, None] // draft_len)
    member_rows = (request_ids >= group_starts[None, :]) & (request_ids < group_ends[None, :])
    chosen = jnp.take(task_emb, group_task, axis=0)
    hyper_out = jax.nn.silu(jnp.dot(chosen, gen_in, preferred_element_type=jnp.float32)).astype(
        jnp.bfloat16
    )
    hyper_width, slab_width, rank_dim = gen_a.shape
    a_local = jnp.einsum(
        "gh,hdr->grd", hyper_out, gen_a, preferred_element_type=jnp.float32
    ).astype(jnp.bfloat16)
    col = lax.axis_index("col")
    own = lax.dynamic_slice_in_dim(flat_tokens, col * slab_width, slab_width, axis=1)
    wide_low = jnp.einsum("grd,td->grt", a_local, own, preferred_element_type=jnp.float32)
    member = member_rows.T.astype(jnp.float32)
    low_part = jnp.sum(wide_low * member[:, None, :], axis=0)
    low_part = low_part.reshape(row_count, rank_dim // row_count, total_rows)
    _, rank_part, ff = gen_b.shape
    b_own = lax.dot_general(
        hyper_out, gen_b, (((1,), (0,)), ((), ())), preferred_element_type=jnp.float32
    ).astype(jnp.bfloat16)
    b_own = b_own.transpose(1, 0, 2).reshape(rank_part * groups, ff)
    model = w_down.shape[1]
    rows = total_rows // chunks
    half = rows // 2
    bf, f32 = jnp.bfloat16, jnp.float32
    dma = pltpu.SemaphoreType.DMA
    y_sems, z_sems = max(ys - 1, 1), max(zs - 1, 1)
    vmem = pl.BlockSpec(memory_space=pltpu.VMEM)
    mixed = pl.pallas_call(
        functools.partial(layer_kernel, row_count, col_count, chunks),
        out_shape=jax.ShapeDtypeStruct((total_rows // col_count, model), bf),
        in_specs=[vmem] * 7,
        out_specs=vmem,
        scratch_shapes=[
            pltpu.VMEM((total_rows, rank_part * groups), bf),
            pltpu.VMEM((row_count - 1, rank_part, total_rows), f32),
            pltpu.VMEM((rank_part, total_rows), f32),
            pltpu.VMEM((col_count - 1, rank_part, total_rows), f32),
            pltpu.VMEM((2 * chunks, rows, ff), f32),
            pltpu.VMEM((2 * chunks, rows, ff), bf),
            pltpu.VMEM((2 * chunks, half, ff), bf),
            pltpu.VMEM((2 * chunks, half, ff), bf),
            pltpu.VMEM((2 * chunks, y_sems, half // ys, ff), bf),
            pltpu.VMEM((chunks, rows, ff), bf),
            pltpu.VMEM((chunks, rows, model), f32),
            pltpu.VMEM((chunks, rows, model), bf),
            pltpu.VMEM((chunks, half, model), bf),
            pltpu.VMEM((chunks, half, model), bf),
            pltpu.VMEM((chunks, z_sems, half // zs, model), bf),
            dma((row_count - 1,)), dma((row_count - 1,)),
            dma((col_count - 1,)), dma((col_count - 1,)),
            dma((2 * chunks,)), dma((2 * chunks,)),
            dma((2 * chunks, y_sems)), dma((2 * chunks, y_sems)),
            dma((chunks, y_sems)), dma((chunks, y_sems)),
            dma((chunks,)), dma((chunks,)),
            dma((chunks,)), dma((chunks,)),
            dma((chunks, z_sems)), dma((chunks, z_sems)),
        ],
        compiler_params=pltpu.CompilerParams(
            collective_id=0, has_side_effects=True, vmem_limit_bytes=60 * 1024 * 1024
        ),
        name="layer",
    )(flat_tokens, low_part, member, b_own, w_gate, w_up, w_down)
    return mixed.reshape(batch_size // col_count, draft_len, model)


def solution(mesh):
    in_specs = (
        P(None, None, "row"),
        P(),
        P(),
        P(None, ("row", "col"), None),
        P(None, "row", "col"),
        P("row", "col"),
        P("row", "col"),
        P("col", "row"),
        P(),
        P(),
    )
    out_specs = P("col", None, "row")
    body = functools.partial(shards, mesh.shape["row"], mesh.shape["col"])
    return jax.shard_map(body, mesh=mesh, in_specs=in_specs, out_specs=out_specs, check_vma=False)
```
